32 devices in a mesh: row: 8 (over z, core), col: 4 (over y, x).
Axes of the slice: x: 2, y: 2, z: 4, core: 2. Of those that a mesh axis runs over, the one named last changes fastest.
Arguments:
- tile_left: bfloat16 [8, 4, 2048, 128], P('row', 'col'), may hold values from -6 to 6
- tile_right: bfloat16 [8, 4, 2048, 128], P('row', 'col'), may hold values from -1 to 1
- tile_blocks: int32 [8, 4], P('row', 'col'), may hold values from 1 to 4
- panel_left: bfloat16 [2, 8, 2048, 128], P(None, 'row', 'col'), may hold values from -6 to 6
- panel_right: bfloat16 [2, 8, 2048, 128], P(None, 'row', 'col'), may hold values from -2 to 2
- swap_flag: int32 [8, 4], P('row', 'col'), may hold values from 0 to 1, as said below
Outputs:
- grown_left: bfloat16 [8, 4, 2048, 256], P('row', 'col')
- grown_right: bfloat16 [8, 4, 2048, 256], P('row', 'col')
The draws below stay inside these ranges and needn't reach their ends.
Inputs may be any that keep to these rules, and one draw needn't show every extreme that they name: swap_flag[i, c] equals swap_flag[i, (c + 4 / 2) mod 4], so tiles change owner in pairs.
All inputs are finite; a program needn't handle non-finite values.
Results may differ from the reference program's by a relative error of at most 0.0057.
Values may be sent and summed in bfloat16 or wider, within the bound.
A program may use at most 64 MiB of HBM per device.

```python
import jax
import jax.numpy as jnp
from jax import lax

NB = 2048
RT = 128
RP = 128
RBLK = 32
N_ROW = 8
N_COL = 4


def draw_swap_flag(key, part):
    halves = jax.random.randint(jax.random.fold_in(key, 7), (N_ROW, N_COL // 2), 0, 2)
    return jnp.concatenate([halves, halves], axis=1).astype(jnp.int32)


def draw_panel_right(key, part):
    spread = 0.4 ** 0.5 * (RP * NB) ** (-0.25)
    shape = (2, N_ROW, NB, RP)
    noise = jnp.clip(jax.random.normal(jax.random.fold_in(key, 13), shape, jnp.float32), -6.0, 6.0) * spread
    stride = NB // RP
    rows = lax_rows = jnp.arange(NB, dtype=jnp.int32)
    cols = jnp.arange(RP, dtype=jnp.int32)
    ident = (rows[:, None] == cols[None, :] * stride).astype(jnp.float32)
    return (noise + ident[None, None]).astype(jnp.bfloat16)


def set_ends(array, key, low, largest):
    extent = array.shape
    index_at = [jax.random.randint(jax.random.fold_in(key, axis), (), 0, extent[axis]) for axis in range(len(extent))]
    array = array.at[tuple(index_at)].set(low)
    longest = extent.index(max(extent))
    index_at[longest] = (index_at[longest] + 1) % extent[longest]
    return array.at[tuple(index_at)].set(largest)


def level_of(rng, shape, pieces, low, top_value):
    loudness, own = 1.0, jax.random.fold_in(rng, 6)
    for position, parts in pieces:
        draws = jnp.exp(jax.random.uniform(jax.random.fold_in(own, position), (parts,), jnp.float32, low / len(pieces), top_value / len(pieces)))
        loudness = loudness * jnp.repeat(draws, shape[position] // parts).reshape([-1 if axis == position else 1 for axis in range(len(shape))])
    return loudness


def bell_draw(key, dims, scale, reach, cuts=(), held_as=jnp.bfloat16):
    entries = jax.random.normal(key, dims, jnp.float32) * scale
    if len(cuts) > 0:
        entries = level_of(key, dims, cuts, -0.22, 0.18) * entries
    return jnp.clip(entries, min=-reach, max=reach).astype(held_as)


def setup_inputs(seed: int = 0) -> dict:
    seeds = jax.random.split(jax.random.key(seed), 7)
    return {
        "tile_left": bell_draw(seeds[0], (N_ROW, N_COL, NB, RT), 1.0, 6.0, ((0, 8), (1, 4))),
        "tile_right": bell_draw(seeds[1], (N_ROW, N_COL, NB, RT), ((2 * RT) ** -0.5), 1.0, ((0, 8), (1, 4))),
        "tile_blocks": set_ends(jax.random.randint(seeds[2], (N_ROW, N_COL), 1, RT // RBLK + 1), jax.random.fold_in(seeds[2], 1), 1, (RT // RBLK + 1) - 1).astype(jnp.int32),
        "panel_left": bell_draw(seeds[3], (2, N_ROW, NB, RP), 1.0, 6.0, ((1, 8), (2, 4))),
        "panel_right": draw_panel_right(jax.random.fold_in(seeds[6], 71), 0),
        "swap_flag": draw_swap_flag(jax.random.fold_in(seeds[6], 71), 0),
    }


def expand(row_left, masked_left, masked_right, col_left, coupling, live_cols):
    lifted = (-jnp.dot(row_left.astype(jnp.float32), coupling.astype(jnp.float32), preferred_element_type=jnp.float32)).astype(jnp.bfloat16)
    stacked_left = jnp.concatenate([masked_left, lifted], axis=1)
    stacked_right = jnp.concatenate([masked_right, col_left], axis=1)
    dead_cols = jnp.concatenate([1.0 - live_cols.astype(jnp.float32), jnp.zeros((coupling.shape[1],), jnp.float32)])
    gram_matrix = jnp.dot(stacked_left.T.astype(jnp.float32), stacked_left.astype(jnp.float32), preferred_element_type=jnp.float32) / stacked_left.shape[0]
    gram_matrix = gram_matrix + jnp.diag(dead_cols)
    factor = jnp.linalg.cholesky(gram_matrix)
    left_out = lax.linalg.triangular_solve(factor, stacked_left.astype(jnp.float32), left_side=False, lower=True, transpose_a=True)
    right_out = jnp.dot(stacked_right.astype(jnp.float32), factor, precision=lax.Precision.HIGHEST)
    return (left_out.astype(jnp.bfloat16), right_out.astype(jnp.bfloat16))

def reference(tile_left, tile_right, tile_blocks, panel_left, panel_right, swap_flag):

    def one_tile(flat_index):
        row_index = flat_index // N_COL
        col_index = flat_index % N_COL
        live_mask = jnp.arange(RT, dtype=jnp.int32) < tile_blocks[row_index, col_index] * RBLK
        zero_value = jnp.zeros((), jnp.bfloat16)
        masked_left = jnp.where(live_mask[None, :], tile_left[row_index, col_index], zero_value)
        masked_right = jnp.where(live_mask[None, :], tile_right[row_index, col_index], zero_value)
        coupling = jnp.dot(panel_right[1, row_index].T.astype(jnp.float32), panel_right[0, col_index].astype(jnp.float32), preferred_element_type=jnp.float32).astype(jnp.bfloat16)
        return expand(panel_left[1, row_index], masked_left, masked_right, panel_left[0, col_index], coupling, live_mask.astype(jnp.float32))
    left_all, right_all = lax.map(one_tile, jnp.arange(N_ROW * N_COL, dtype=jnp.int32))
    left_all = left_all.reshape(N_ROW, N_COL, NB, RT + RP)
    right_all = right_all.reshape(N_ROW, N_COL, NB, RT + RP)
    chosen = (swap_flag == 1)[:, :, None, None]
    grown_left = jnp.where(chosen, jnp.roll(left_all, N_COL // 2, axis=1), left_all)
    grown_right = jnp.where(chosen, jnp.roll(right_all, N_COL // 2, axis=1), right_all)
    return (grown_left, grown_right)
```

```python
import functools

import jax
import jax.numpy as jnp
from jax import lax
from jax.experimental import pallas as pl
from jax.experimental.pallas import tpu as pltpu
from jax.sharding import PartitionSpec as P

RBLK = 32
MESH = pl.DeviceIdType.MESH
BF16 = jnp.bfloat16
F32 = jnp.float32
TN = (((0,), (0,)), ((), ()))
NT = (((1,), (1,)), ((), ()))


def update(R, C, NV, u, v, pleft, pright, blocks, swap, lo, ro,
           ubuf, vbuf, uown, vown, pr1, rowbuf, colbuf, prbuf, part, psend, precv, mine, mbuf, stack, work, sblk, sswp,
           s_u, r_u, s_v, r_v, s_row, r_row, s_fwd, s_col, r_col, s_st, s_pr, r_pr, s_part, r_part, s_meta, r_meta,
           s_loc):
    r, c = lax.axis_index("row"), lax.axis_index("col")
    half = C // 2
    mate = lax.rem(c + half, C)
    sib = r + 1 - 2 * lax.rem(r, 2)
    has_up, has_dn = r + 2 < R, r >= 2
    nb, rk = u.shape
    blk, rp = pleft.shape[1:]
    n = rk + rp
    tiles = (c, mate)

    def rcopy(src, dst, ss, rs, to):
        return pltpu.make_async_remote_copy(
            src_ref=src, dst_ref=dst, send_sem=ss, recv_sem=rs, device_id=to, device_id_type=MESH
        )

    load_b = pltpu.make_async_copy(blocks, sblk, s_loc.at[0])
    load_s = pltpu.make_async_copy(swap, sswp, s_loc.at[1])
    load_r = pltpu.make_async_copy(pright.at[1], pr1, s_loc.at[2])
    load_l = pltpu.make_async_copy(pleft.at[1], rowbuf.at[c], s_loc.at[3])
    load_u = pltpu.make_async_copy(u, uown, s_loc.at[4])
    load_v = pltpu.make_async_copy(v, vown, s_loc.at[5])
    load_p = pltpu.make_async_copy(pright.at[0], prbuf.at[lax.min(r, C - 1)], s_loc.at[6])
    load_c = [pltpu.make_async_copy(pleft.at[0], colbuf.at[t, c], s_loc.at[7 + t]) for t in range(2)]
    for copy in (load_b, load_s, load_r, load_l, load_u, load_v):
        copy.start()

    @pl.when(r < C)
    def _():
        load_p.start()

    for t in range(2):
        @pl.when(r == tiles[t])
        def _():
            load_c[t].start()

    barrier = pltpu.get_barrier_semaphore()
    for d in range(C):
        @pl.when(d != c)
        def _():
            pl.semaphore_signal(barrier, inc=1, device_id=(r, d), device_id_type=MESH)
    pl.semaphore_signal(barrier, inc=1, device_id=(sib, c), device_id_type=MESH)

    @pl.when(has_up)
    def _():
        pl.semaphore_signal(barrier, inc=1, device_id=(r + 2, c), device_id_type=MESH)

    @pl.when(has_dn)
    def _():
        pl.semaphore_signal(barrier, inc=1, device_id=(r - 2, c), device_id_type=MESH)

    load_b.wait()
    load_s.wait()
    top = lax.broadcasted_iota(jnp.int32, (8, 128), 0) == 0
    own_meta = jnp.where(top, sswp[0, 0], sblk[0, 0]).astype(F32)
    mine[...] = own_meta
    pl.semaphore_wait(barrier, C + jnp.where(has_up, 1, 0) + jnp.where(has_dn, 1, 0))

    ends = []

    def send(cond, copy):
        @pl.when(cond)
        def _():
            copy.start()
        ends.append((cond, copy))

    for d in range(C):
        send(c != d, rcopy(mine, mbuf.at[c], s_meta.at[d], r_meta.at[c], (r, d)))
    at_r = lax.min(r, C - 1)
    own_pr = (prbuf.at[at_r], s_pr.at[at_r], r_pr.at[at_r])
    for k, (cond, to) in enumerate(((has_up, r + 2), (has_dn, r - 2), (True, sib))):
        send((r < C) & cond, rcopy(pright.at[0], own_pr[0], own_pr[1].at[k], own_pr[2], (to, c)))
    for d in range(C):
        send((c != d) & (mate == d), rcopy(pleft.at[1], rowbuf.at[c], s_row.at[d], r_row.at[c], (r, d)))
    for d in range(C):
        same = (c // half) == d // half
        send((c != d) & same & (mate != d), rcopy(pleft.at[1], rowbuf.at[c], s_row.at[d], r_row.at[c], (r, d)))
    for t in range(2):
        d = lax.rem(r + t * half, C)
        send((r < C) & (d != c), rcopy(pleft.at[0], colbuf.at[t, c], s_st.at[t], r_col.at[t, c], (r, d)))

    for t in range(2):
        slot, rs, ss = colbuf.at[t, c], r_col.at[t, c], s_col.at[t, c]
        for k, (cond, to) in enumerate(((has_up, r + 2), (has_dn, r - 2), (True, sib))):
            send((r == tiles[t]) & cond, rcopy(pleft.at[0], slot, ss.at[k], rs, (to, c)))
    swap_u = rcopy(u, ubuf, s_u, r_u, (r, mate))
    swap_u.start()

    load_r.wait()

    @pl.when(r < C)
    def _():
        load_p.wait()

    def forward_row():
        rcopy(pleft.at[1], rowbuf.at[mate], s_row.at[0], r_row.at[mate], (r, mate)).wait_recv()
        for d in range(C):
            same = (c // half) == d // half
            send((c != d) & same, rcopy(rowbuf.at[mate], rowbuf.at[mate], s_fwd.at[d], r_row.at[mate], (r, d)))

    pairs = C // 2
    near = [2 * jnp.where(r // 2 + k < pairs, r // 2 + k, pairs - 1 - k) for k in range(pairs)]
    for w in range(2):
        for k in range(pairs):
            s = near[k] + lax.rem(r + w, 2)
            slot, rs, ss = prbuf.at[s], r_pr.at[s], s_pr.at[s]

            @pl.when(r != s)
            def _():
                rcopy(slot, slot, ss.at[0], rs, (sib, c)).wait_recv()

            if w == 0:
                send((r > s) & has_up, rcopy(slot, slot, ss.at[0], rs, (r + 2, c)))
                send((r < s) & has_dn, rcopy(slot, slot, ss.at[1], rs, (r - 2, c)))
                send(r != s, rcopy(slot, slot, ss.at[2], rs, (sib, c)))
            part[s] = lax.dot_general(pr1[...], prbuf[s], TN, preferred_element_type=F32)
        if w == 0:
            forward_row()

    for d in range(C):
        @pl.when(c != d)
        def _():
            rcopy(mine, mbuf.at[d], s_meta.at[d], r_meta.at[d], (r, d)).wait_recv()

        @pl.when(c == d)
        def _():
            mbuf[d] = own_meta

    flagged = own_meta[0:1, :] > 0.5
    for d in range(C):
        psend[d] = jnp.where(mbuf[d][0:1, :] > 0.5, part[(d + half) % C], part[d]).astype(BF16)
    total = jnp.where(flagged, part[mate], part[c])
    for d in range(C):
        send((c != d) & (mate == d), rcopy(psend.at[d], precv.at[c], s_part.at[d], r_part.at[c], (r, d)))
    for d in range(C):
        send((c != d) & (mate != d), rcopy(psend.at[d], precv.at[c], s_part.at[d], r_part.at[c], (r, d)))

    vb = nb // NV
    swap_v = [rcopy(v.at[pl.ds(k * vb, vb)], vbuf.at[pl.ds(k * vb, vb)], s_v.at[k], r_v.at[k], (r, mate))
              for k in range(NV)]
    for copy in swap_v:
        copy.start()

    def away(t):
        return jnp.abs(r // 2 - tiles[t] // 2)

    first = jnp.where(away(1) < away(0), 1, 0)
    for t in (first, 1 - first):
        home = jnp.where(t == 0, c, mate)
        par = lax.rem(r, 2) == lax.rem(home, 2)
        for k in range(C):
            b = lax.rem(c + k, half) + half * lax.rem(c // half + k // half, 2)
            slot, rs, ss = colbuf.at[t, b], r_col.at[t, b], s_col.at[t, b]
            relay = par & ((r != home) | (c != b))

            @pl.when(relay)
            def _():
                rcopy(slot, slot, ss.at[0], rs, (sib, c)).wait_recv()

            send(relay & (r >= home) & has_up, rcopy(slot, slot, ss.at[0], rs, (r + 2, c)))
            send(relay & (r <= home) & has_dn, rcopy(slot, slot, ss.at[1], rs, (r - 2, c)))
            send(relay, rcopy(slot, slot, ss.at[2], rs, (sib, c)))

    chosen_meta = jnp.where(flagged, mbuf[mate], own_meta)
    lane = lax.broadcasted_iota(jnp.int32, (1, rk), 1).astype(F32)
    live = lane < chosen_meta[1:2, :] * RBLK
    zero = jnp.zeros((), BF16)

    load_l.wait()
    for d in range(C):
        @pl.when((c != d) & (mate != d))
        def _():
            rcopy(pleft.at[1], rowbuf.at[d], s_row.at[d], r_row.at[d], (r, d)).wait_recv()
    load_u.wait()
    swap_u.wait_recv()
    for d in range(C):
        @pl.when(c != d)
        def _():
            rcopy(psend.at[d], precv.at[d], s_part.at[d], r_part.at[d], (r, d)).wait_recv()

        @pl.when(c == d)
        def _():
            precv[d] = jnp.zeros((rp, rp), BF16)
    for d in range(C):
        total = total + precv[d].astype(F32)
    coup = total.astype(BF16)

    def fill(step, acc):
        at = pl.ds(pl.multiple_of(step * blk, blk), blk)
        lifted = -jnp.dot(rowbuf[step], coup, preferred_element_type=F32)
        left = jnp.where(flagged, ubuf[at, :], uown[at, :])
        piece = jnp.concatenate([jnp.where(live, left, zero), lifted.astype(BF16)], axis=1)
        stack[at, :] = piece
        return acc + lax.dot_general(piece, piece, TN, preferred_element_type=F32)

    gram = lax.fori_loop(0, C, fill, jnp.zeros((n, n), F32)) / nb
    ri = lax.broadcasted_iota(jnp.int32, (n, n), 0)
    ci = lax.broadcasted_iota(jnp.int32, (n, n), 1)
    dead = jnp.concatenate([jnp.where(live, 0.0, 1.0).astype(F32), jnp.zeros((1, rp), F32)], axis=1)
    work[:, :n] = gram + jnp.where(ri == ci, dead, 0.0)
    work[:, n:] = jnp.where(ri == ci, 1.0, 0.0).astype(F32)
    factor_rows(work, n, 32)
    uph, upm, _ = split3(jnp.where(ri <= ci, work[:, :n], 0.0))
    inh, inm, _ = split3(work[:, n:])

    def product(value, high, low):
        out = lax.dot_general(value, high, NT, preferred_element_type=F32)
        return (out + lax.dot_general(value, low, NT, preferred_element_type=F32)).astype(BF16)

    def left_step(step, _):
        at = pl.ds(pl.multiple_of(step * vb, vb), vb)
        lo[at, :] = product(stack[at, :], inh, inm)
        return 0

    lax.fori_loop(0, NV, left_step, 0)

    load_v.wait()
    for t in range(2):
        @pl.when(r == tiles[t])
        def _():
            load_c[t].wait()

        for b in range(C):
            @pl.when(lax.rem(r, 2) != lax.rem(tiles[t], 2))
            def _():
                rcopy(colbuf.at[t, b], colbuf.at[t, b], s_col.at[t, b, 0], r_col.at[t, b], (sib, c)).wait_recv()

    for k in range(NV):
        swap_v[k].wait_recv()
        at = pl.ds(k * vb, vb)
        right = jnp.where(live, jnp.where(flagged, vbuf[at, :], vown[at, :]), zero)
        first, count = k * vb // blk, max(vb // blk, 1)
        cols = pl.ds(k * vb % blk, min(vb, blk))
        own = [jnp.where(flagged, colbuf[1, first + i, cols, :], colbuf[0, first + i, cols, :]) for i in range(count)]
        pair = jnp.concatenate([right, jnp.concatenate(own, axis=0)], axis=1)
        ro[at, :] = product(pair, uph, upm)

    swap_u.wait_send()
    for copy in swap_v:
        copy.wait_send()
    for cond, copy in ends:
        @pl.when(cond)
        def _():
            copy.wait_send()


def split3(x):
    h = x.astype(BF16)
    rest = x - h.astype(F32)
    m = rest.astype(BF16)
    return h, m, (rest - m.astype(F32)).astype(BF16)


def factor_rows(work, n, sb):
    lanes = 128
    sub = lax.broadcasted_iota(jnp.int32, (8, lanes), 0)
    groups = sb // 8

    def sub_row(x, k):
        return jnp.broadcast_to(x[k : k + 1, :], x.shape)

    for r0 in range(0, n, sb):
        a0 = r0 // lanes * lanes
        width = n + lanes
        tiles = width // lanes
        rows = [
            [work[r0 + 8 * g : r0 + 8 * g + 8, a0 + lanes * w : a0 + lanes * (w + 1)] for w in range(tiles)]
            for g in range(groups)
        ]
        for t in range(groups):
            base = r0 - a0 + 8 * t
            cols = [
                {g: jnp.broadcast_to(rows[g][0][:, base + i : base + i + 1], (8, lanes)) for g in range(t, groups)}
                for i in range(8)
            ]
            for k in range(8):
                inv = lax.rsqrt(sub_row(cols[k][t], k))
                scaled = {g: cols[k][g] * inv for g in range(t, groups)}
                for j in range(k + 1, 8):
                    lj = sub_row(scaled[t], j)
                    for g in range(t, groups):
                        cols[j][g] = cols[j][g] - scaled[g] * lj
                below = jnp.where(sub > k, scaled[t], 0.0)
                for w in range(tiles):
                    rowk = sub_row(rows[t][w], k) * inv
                    rows[t][w] = jnp.where(sub == k, rowk, rows[t][w] - below * rowk)
                    for g in range(t + 1, groups):
                        rows[g][w] = rows[g][w] - scaled[g] * rowk
        done = jnp.concatenate([jnp.concatenate(rows[g], axis=1) for g in range(groups)], axis=0)
        work[r0 : r0 + sb, a0 : a0 + width] = done
        r1 = r0 + sb
        if r1 < n:
            b0 = r1 // lanes * lanes
            h, m, l = split3(done)
            left = jnp.concatenate([h, h, m, m, h, l], axis=0)[:, b0 - a0 : n - a0]
            right = jnp.concatenate([h, m, h, m, l, h], axis=0)
            update = lax.dot_general(left, right, (((0,), (0,)), ((), ())), preferred_element_type=F32)
            work[r1:n, a0 : a0 + width] = work[r1:n, a0 : a0 + width] - update[r1 - b0 :, :]


def per_device(R, C, tile_left, tile_right, tile_blocks, panel_left, panel_right, swap_flag):
    nb, rk = tile_left.shape[2:]
    blk, rp = panel_left.shape[2:]
    n = rk + rp
    NV = 4
    vm = pl.BlockSpec(memory_space=pltpu.VMEM)
    hbm = pl.BlockSpec(memory_space=pltpu.HBM)
    dma = pltpu.SemaphoreType.DMA
    S = jax.ShapeDtypeStruct
    V = pltpu.VMEM
    lo, ro = pl.pallas_call(
        functools.partial(update, R, C, NV),
        out_shape=(S((nb, n), BF16),) * 2,
        in_specs=[hbm] * 6,
        out_specs=[vm] * 2,
        scratch_shapes=[
            V((nb, rk), BF16), V((nb, rk), BF16), V((nb, rk), BF16), V((nb, rk), BF16), V((blk, rp), BF16),
            V((C, blk, rp), BF16), V((2, C, blk, rp), BF16), V((C, blk, rp), BF16),
            V((C, rp, rp), F32), V((C, rp, rp), BF16), V((C, rp, rp), BF16), V((8, 128), F32), V((C, 8, 128), F32),
            V((nb, n), BF16), V((n, 2 * n), F32), pltpu.SMEM((1, 1), jnp.int32), pltpu.SMEM((1, 1), jnp.int32),
            dma, dma, dma((NV,)), dma((NV,)), dma((C,)), dma((C,)), dma((C,)), dma((2, C, 3)), dma((2, C)), dma((2,)),
            dma((C, 3)), dma((C,)), dma((C,)), dma((C,)), dma((C,)), dma((C,)), dma((9,)),
        ],
        compiler_params=pltpu.CompilerParams(
            collective_id=0, has_side_effects=True, vmem_limit_bytes=58 * 1024 * 1024
        ),
        name="update",
    )(tile_left[0, 0], tile_right[0, 0], panel_left[:, 0], panel_right[:, 0], tile_blocks, swap_flag)
    return lo[None, None], ro[None, None]


def solution(mesh):
    placed = (
        P("row", "col", None, None),
        P("row", "col", None, None),
        P("row", "col"),
        P(None, "row", "col", None),
        P(None, "row", "col", None),
        P("row", "col"),
    )
    return jax.shard_map(
        functools.partial(per_device, mesh.shape["row"], mesh.shape["col"]),
        mesh=mesh,
        in_specs=placed,
        out_specs=(P("row", "col", None, None), P("row", "col", None, None)),
        check_vma=False,
    )
```

```python
import functools

import jax
import jax.numpy as jnp
from jax import lax
from jax.experimental import pallas as pl
from jax.experimental.pallas import tpu as pltpu
from jax.sharding import PartitionSpec as P

RBLK = 32
MESH = pl.DeviceIdType.MESH
BF16 = jnp.bfloat16
F32 = jnp.float32
TN = (((0,), (0,)), ((), ()))
NT = (((1,), (1,)), ((), ()))
NN = (((1,), (0,)), ((), ()))


def update(R, C, u, v, pleft, pright, blocks, swap, lo, ro,
           ubuf, vbuf, uown, vown, pr1, rowbuf, colbuf, prbuf, part, psend, precv, mine, mbuf, stack, work, sblk, sswp,
           s_u, r_u, s_v, r_v, s_row, r_row, s_fwd, s_col, r_col, s_st, s_pr, r_pr, s_part, r_part, s_meta, r_meta,
           s_loc):
    r, c = lax.axis_index("row"), lax.axis_index("col")
    half = C // 2
    mate = lax.rem(c + half, C)
    sib = r + 1 - 2 * lax.rem(r, 2)
    has_up, has_dn = r + 2 < R, r >= 2
    nb, rk = u.shape
    blk, rp = pleft.shape[1:]
    n = rk + rp
    tiles = (c, mate)

    def nth(dev, k):
        return lax.rem(dev + k, half) + half * lax.rem(dev // half + k // half, 2)

    def rcopy(src, dst, ss, rs, to):
        return pltpu.make_async_remote_copy(
            src_ref=src, dst_ref=dst, send_sem=ss, recv_sem=rs, device_id=to, device_id_type=MESH
        )

    load_b = pltpu.make_async_copy(blocks, sblk, s_loc.at[0])
    load_s = pltpu.make_async_copy(swap, sswp, s_loc.at[1])
    load_r = pltpu.make_async_copy(pright.at[1], pr1, s_loc.at[2])
    load_l = pltpu.make_async_copy(pleft.at[1], rowbuf.at[c], s_loc.at[3])
    load_u = pltpu.make_async_copy(u, uown, s_loc.at[4])
    load_v = pltpu.make_async_copy(v, vown, s_loc.at[5])
    load_p = pltpu.make_async_copy(pright.at[0], prbuf.at[lax.min(r, C - 1)], s_loc.at[6])
    load_c = [pltpu.make_async_copy(pleft.at[0], colbuf.at[t, c], s_loc.at[7 + t]) for t in range(2)]
    for copy in (load_b, load_s, load_r, load_l, load_u, load_v):
        copy.start()

    @pl.when(r < C)
    def _():
        load_p.start()

    for t in range(2):
        @pl.when(r == tiles[t])
        def _():
            load_c[t].start()

    barrier = pltpu.get_barrier_semaphore()
    for d in range(C):
        @pl.when(d != c)
        def _():
            pl.semaphore_signal(barrier, inc=1, device_id=(r, d), device_id_type=MESH)
    pl.semaphore_signal(barrier, inc=1, device_id=(sib, c), device_id_type=MESH)

    @pl.when(has_up)
    def _():
        pl.semaphore_signal(barrier, inc=1, device_id=(r + 2, c), device_id_type=MESH)

    @pl.when(has_dn)
    def _():
        pl.semaphore_signal(barrier, inc=1, device_id=(r - 2, c), device_id_type=MESH)

    load_b.wait()
    load_s.wait()
    top = lax.broadcasted_iota(jnp.int32, (8, 128), 0) == 0
    own_meta = jnp.where(top, sswp[0, 0], sblk[0, 0]).astype(F32)
    mine[...] = own_meta
    pl.semaphore_wait(barrier, C + jnp.where(has_up, 1, 0) + jnp.where(has_dn, 1, 0))

    ends = []

    def send(cond, copy):
        @pl.when(cond)
        def _():
            copy.start()
        ends.append((cond, copy))

    for d in range(C):
        send(c != d, rcopy(mine, mbuf.at[c], s_meta.at[d], r_meta.at[c], (r, d)))
    at_r = lax.min(r, C - 1)
    own_pr = (prbuf.at[at_r], s_pr.at[at_r], r_pr.at[at_r])
    for k, (cond, to) in enumerate(((has_up, r + 2), (has_dn, r - 2), (True, sib))):
        send((r < C) & cond, rcopy(pright.at[0], own_pr[0], own_pr[1].at[k], own_pr[2], (to, c)))
    for t in range(2):
        d = lax.rem(r + t * half, C)
        send((r < C) & (d != c), rcopy(pleft.at[0], colbuf.at[t, c], s_st.at[t], r_col.at[t, c], (r, d)))

    for d in range(C):
        same = (c // half) == d // half
        send((c != d) & same & (mate != d), rcopy(pleft.at[1], rowbuf.at[c], s_row.at[d], r_row.at[c], (r, d)))
    swap_u = rcopy(u, ubuf, s_u, r_u, (r, mate))
    swap_u.start()
    for d in range(C):
        send((c != d) & (mate == d), rcopy(pleft.at[1], rowbuf.at[c], s_row.at[d], r_row.at[c], (r, d)))

    load_r.wait()

    @pl.when(r < C)
    def _():
        load_p.wait()

    def forward_row():
        rcopy(pleft.at[1], rowbuf.at[mate], s_row.at[0], r_row.at[mate], (r, mate)).wait_recv()
        for d in range(C):
            same = (c // half) == d // half
            send((c != d) & same, rcopy(rowbuf.at[mate], rowbuf.at[mate], s_fwd.at[d], r_row.at[mate], (r, d)))

    pairs = C // 2
    near = [2 * jnp.where(r // 2 + k < pairs, r // 2 + k, pairs - 1 - k) for k in range(pairs)]
    for w in range(2):
        for k in range(pairs):
            s = near[k] + lax.rem(r + w, 2)
            slot, rs, ss = prbuf.at[s], r_pr.at[s], s_pr.at[s]

            @pl.when(r != s)
            def _():
                rcopy(slot, slot, ss.at[0], rs, (sib, c)).wait_recv()

            if w == 0:
                send((r > s) & has_up, rcopy(slot, slot, ss.at[0], rs, (r + 2, c)))
                send((r < s) & has_dn, rcopy(slot, slot, ss.at[1], rs, (r - 2, c)))
                send(r != s, rcopy(slot, slot, ss.at[2], rs, (sib, c)))
            part[s] = lax.dot_general(pr1[...], prbuf[s], TN, preferred_element_type=F32)
        if w == 0:
            for t in range(2):
                slot, rs, ss = colbuf.at[t, c], r_col.at[t, c], s_col.at[t, c]
                for k, (cond, to) in enumerate(((has_up, r + 2), (has_dn, r - 2), (True, sib))):
                    send((r == tiles[t]) & cond, rcopy(pleft.at[0], slot, ss.at[k], rs, (to, c)))

    for d in range(C):
        @pl.when(c != d)
        def _():
            rcopy(mine, mbuf.at[d], s_meta.at[d], r_meta.at[d], (r, d)).wait_recv()

        @pl.when(c == d)
        def _():
            mbuf[d] = own_meta

    flagged = own_meta[0:1, :] > 0.5
    for d in range(C):
        psend[d] = jnp.where(mbuf[d][0:1, :] > 0.5, part[(d + half) % C], part[d]).astype(BF16)
    total = jnp.where(flagged, part[mate], part[c])
    for d in range(C):
        send((c != d) & (mate == d), rcopy(psend.at[d], precv.at[c], s_part.at[d], r_part.at[c], (r, d)))
    for d in range(C):
        send((c != d) & (mate != d), rcopy(psend.at[d], precv.at[c], s_part.at[d], r_part.at[c], (r, d)))

    def v_chunk(b):
        at = pl.ds(pl.multiple_of(b * blk, blk), blk)
        return rcopy(v.at[at], vbuf.at[at], s_v.at[b], r_v.at[b], (r, mate))

    for k in range(C):
        v_chunk(nth(mate, k)).start()

    def away(t):
        return jnp.abs(r // 2 - tiles[t] // 2)

    near_t = jnp.where(away(1) < away(0), 1, 0)
    far_t = 1 - near_t
    far_home = jnp.where(far_t == 0, c, mate)
    far_away = jnp.abs(r // 2 - far_home // 2)
    early = far_away <= 1
    ending = jnp.logical_not(early) & jnp.where(r > far_home, jnp.logical_not(has_up), jnp.logical_not(has_dn))

    def pass_on(t, k, now):
        home = jnp.where(t == 0, c, mate)
        b = nth(c, k)
        slot, rs, ss = colbuf.at[t, b], r_col.at[t, b], s_col.at[t, b]
        relay = (lax.rem(r, 2) == lax.rem(home, 2)) & ((r != home) | (c != b)) & now

        @pl.when(relay)
        def _():
            rcopy(slot, slot, ss.at[0], rs, (sib, c)).wait_recv()

        send(relay & (r >= home) & has_up, rcopy(slot, slot, ss.at[0], rs, (r + 2, c)))
        send(relay & (r <= home) & has_dn, rcopy(slot, slot, ss.at[1], rs, (r - 2, c)))
        send(relay, rcopy(slot, slot, ss.at[2], rs, (sib, c)))

    for k in range(C):
        pass_on(near_t, k, True)
    for k in range(C):
        pass_on(far_t, k, early)
    inside = jnp.logical_not(early | ending)

    chosen_meta = jnp.where(flagged, mbuf[mate], own_meta)
    lane = lax.broadcasted_iota(jnp.int32, (1, rk), 1).astype(F32)
    live = lane < chosen_meta[1:2, :] * RBLK
    zero = jnp.zeros((), BF16)

    def sliced(step):
        return pl.ds(pl.multiple_of(step * blk, blk), blk)

    load_u.wait()
    swap_u.wait_recv()

    def fill(step, acc):
        left = jnp.where(live, jnp.where(flagged, ubuf[sliced(step), :], uown[sliced(step), :]), zero)
        stack[sliced(step), :rk] = left
        return acc + lax.dot_general(left, left, TN, preferred_element_type=F32)

    g11 = lax.fori_loop(0, C, fill, jnp.zeros((rk, rk), F32), unroll=True) / nb
    dead = jnp.where(live, 0.0, 1.0).astype(F32)
    eye = jnp.where(
        lax.broadcasted_iota(jnp.int32, (rk, rk), 0) == lax.broadcasted_iota(jnp.int32, (rk, rk), 1), 1.0, 0.0
    ).astype(F32)
    work[:, :rk] = g11 + eye * dead
    work[:, rk:] = eye
    factor_rows(work, rk, 64)
    forward_row()
    pass_on(far_t, 0, inside)
    upper = jnp.where(
        lax.broadcasted_iota(jnp.int32, (rk, rk), 0) <= lax.broadcasted_iota(jnp.int32, (rk, rk), 1), 1.0, 0.0
    ).astype(F32)
    u11, i11 = work[:, :rk] * upper, work[:, rk:]

    load_l.wait()
    for d in range(C):
        @pl.when((c != d) & (mate != d))
        def _():
            rcopy(pleft.at[1], rowbuf.at[d], s_row.at[d], r_row.at[d], (r, d)).wait_recv()
    for d in range(C):
        @pl.when(c != d)
        def _():
            rcopy(psend.at[d], precv.at[d], s_part.at[d], r_part.at[d], (r, d)).wait_recv()

        @pl.when(c == d)
        def _():
            precv[d] = jnp.zeros((rp, rp), BF16)
    for d in range(C):
        total = total + precv[d].astype(F32)
    coup = total.astype(BF16)

    def lift(step, acc):
        lifted = (-jnp.dot(rowbuf[step], coup, preferred_element_type=F32)).astype(BF16)
        stack[sliced(step), rk:] = lifted
        return acc + lax.dot_general(stack[sliced(step), :], lifted, TN, preferred_element_type=F32)

    g2 = lax.fori_loop(0, C, lift, jnp.zeros((n, rp), F32), unroll=True) / nb
    pass_on(far_t, 1, inside)

    def exact(x, y, dims):
        return lax.dot_general(x, y, dims, precision=lax.Precision.HIGHEST, preferred_element_type=F32)

    u12 = exact(i11, g2[:rk, :], NN)
    work[:, :rp] = g2[rk:, :] - exact(u12, u12, TN)
    work[:, rp:] = eye
    factor_rows(work, rp, 64)
    pass_on(far_t, 2, inside)
    u22, i22 = work[:, :rp] * upper, work[:, rp:]
    i21 = -exact(i22, exact(u12, i11, TN), NN)
    none = jnp.zeros((rk, rp), F32)
    uph, upm, _ = split3(jnp.concatenate(
        [jnp.concatenate([u11, u12], axis=1), jnp.concatenate([none, u22], axis=1)], axis=0))
    inh, inm, _ = split3(jnp.concatenate(
        [jnp.concatenate([i11, none], axis=1), jnp.concatenate([i21, i22], axis=1)], axis=0))
    pass_on(far_t, 3, inside)
    for k in range(4, C):
        pass_on(far_t, k, inside)

    def product(value, high, low):
        out = lax.dot_general(value, high, NT, preferred_element_type=F32)
        return (out + lax.dot_general(value, low, NT, preferred_element_type=F32)).astype(BF16)

    lo[...] = product(stack[...], inh, inm)
    for k in range(C):
        pass_on(far_t, k, ending)

    load_v.wait()
    for t in range(2):
        @pl.when(r == tiles[t])
        def _():
            load_c[t].wait()
    def arrived(k):
        b = nth(c, k)
        for t in range(2):
            @pl.when(lax.rem(r, 2) != lax.rem(tiles[t], 2))
            def _():
                rcopy(colbuf.at[t, b], colbuf.at[t, b], s_col.at[t, b, 0], r_col.at[t, b], (sib, c)).wait_recv()
        v_chunk(b).wait_recv()

    def right_rows(k):
        b = nth(c, k)
        right = jnp.where(live, jnp.where(flagged, vbuf[sliced(b), :], vown[sliced(b), :]), zero)
        own = jnp.where(flagged, colbuf[1, b], colbuf[0, b])
        return jnp.concatenate([right, own], axis=1)

    for group in (range(C - 1), range(C - 1, C)):
        for k in group:
            arrived(k)
        out = product(jnp.concatenate([right_rows(k) for k in group], axis=0), uph, upm)
        for i, k in enumerate(group):
            ro[sliced(nth(c, k)), :] = out[i * blk : (i + 1) * blk, :]

    for b in range(C):
        v_chunk(b).wait_send()
    swap_u.wait_send()
    for cond, copy in ends:
        @pl.when(cond)
        def _():
            copy.wait_send()


def split3(x):
    h = x.astype(BF16)
    rest = x - h.astype(F32)
    m = rest.astype(BF16)
    return h, m, (rest - m.astype(F32)).astype(BF16)


def factor_rows(work, n, sb):
    lanes = 128
    sub = lax.broadcasted_iota(jnp.int32, (8, lanes), 0)
    groups = sb // 8

    def sub_row(x, k):
        return jnp.broadcast_to(x[k : k + 1, :], x.shape)

    for r0 in range(0, n, sb):
        a0 = r0 // lanes * lanes
        width = n + lanes
        tiles = width // lanes
        rows = [
            [work[r0 + 8 * g : r0 + 8 * g + 8, a0 + lanes * w : a0 + lanes * (w + 1)] for w in range(tiles)]
            for g in range(groups)
        ]
        for t in range(groups):
            base = r0 - a0 + 8 * t
            cols = [
                {g: jnp.broadcast_to(rows[g][0][:, base + i : base + i + 1], (8, lanes)) for g in range(t, groups)}
                for i in range(8)
            ]
            for k in range(8):
                inv = lax.rsqrt(sub_row(cols[k][t], k))
                scaled = {g: cols[k][g] * inv for g in range(t, groups)}
                for j in range(k + 1, 8):
                    lj = sub_row(scaled[t], j)
                    for g in range(t, groups):
                        cols[j][g] = cols[j][g] - scaled[g] * lj
                below = jnp.where(sub > k, scaled[t], 0.0)
                for w in range(tiles):
                    rowk = sub_row(rows[t][w], k) * inv
                    rows[t][w] = jnp.where(sub == k, rowk, rows[t][w] - below * rowk)
                    for g in range(t + 1, groups):
                        rows[g][w] = rows[g][w] - scaled[g] * rowk
        done = jnp.concatenate([jnp.concatenate(rows[g], axis=1) for g in range(groups)], axis=0)
        work[r0 : r0 + sb, a0 : a0 + width] = done
        r1 = r0 + sb
        if r1 < n:
            b0 = r1 // lanes * lanes
            h, m, l = split3(done)
            left = jnp.concatenate([h, h, m, m, h, l], axis=0)[:, b0 - a0 : n - a0]
            right = jnp.concatenate([h, m, h, m, l, h], axis=0)
            update = lax.dot_general(left, right, (((0,), (0,)), ((), ())), preferred_element_type=F32)
            work[r1:n, a0 : a0 + width] = work[r1:n, a0 : a0 + width] - update[r1 - b0 :, :]


def per_device(R, C, tile_left, tile_right, tile_blocks, panel_left, panel_right, swap_flag):
    nb, rk = tile_left.shape[2:]
    blk, rp = panel_left.shape[2:]
    n = rk + rp
    vm = pl.BlockSpec(memory_space=pltpu.VMEM)
    hbm = pl.BlockSpec(memory_space=pltpu.HBM)
    dma = pltpu.SemaphoreType.DMA
    V = pltpu.VMEM
    lo, ro = pl.pallas_call(
        functools.partial(update, R, C),
        out_shape=(pltpu.VMEM((nb, n), BF16),) * 2,
        in_specs=[hbm] * 6,
        out_specs=[vm] * 2,
        scratch_shapes=[
            V((nb, rk), BF16), V((nb, rk), BF16), V((nb, rk), BF16), V((nb, rk), BF16), V((blk, rp), BF16),
            V((C, blk, rp), BF16), V((2, C, blk, rp), BF16), V((C, blk, rp), BF16),
            V((C, rp, rp), F32), V((C, rp, rp), BF16), V((C, rp, rp), BF16), V((8, 128), F32), V((C, 8, 128), F32),
            V((nb, n), BF16), V((rk, 2 * rk), F32), pltpu.SMEM((1, 1), jnp.int32), pltpu.SMEM((1, 1), jnp.int32),
            dma, dma, dma((C,)), dma((C,)), dma((C,)), dma((C,)), dma((C,)), dma((2, C, 3)), dma((2, C)), dma((2,)),
            dma((C, 3)), dma((C,)), dma((C,)), dma((C,)), dma((C,)), dma((C,)), dma((9,)),
        ],
        compiler_params=pltpu.CompilerParams(
            collective_id=0, has_side_effects=True, vmem_limit_bytes=58 * 1024 * 1024
        ),
        name="update",
    )(tile_left[0, 0], tile_right[0, 0], panel_left[:, 0], panel_right[:, 0], tile_blocks, swap_flag)
    return lo[None, None], ro[None, None]


def solution(mesh):
    placed = (
        P("row", "col", None, None),
        P("row", "col", None, None),
        P("row", "col"),
        P(None, "row", "col", None),
        P(None, "row", "col", None),
        P("row", "col"),
    )
    return jax.shard_map(
        functools.partial(per_device, mesh.shape["row"], mesh.shape["col"]),
        mesh=mesh,
        in_specs=placed,
        out_specs=(P("row", "col", None, None), P("row", "col", None, None)),
        check_vma=False,
    )
```
